32 devices in a mesh: group: 4 (over y, x), dp: 8 (over z, core).
Axes of the slice: x: 2, y: 2, z: 4, core: 2. Of those that a mesh axis runs over, the one named last changes fastest.
Arguments:
- observations: bfloat16 [64, 64, 4096], P('dp', None, 'group'), may hold values from -6 to 6
- next_observations: bfloat16 [1024, 4096], P('dp', 'group'), may hold values from -6 to 6
- trunk_weights: bfloat16 [2, 4096, 4096], P(None, 'dp', 'group'), may hold values from -0.125 to 0.125
- head_weights: bfloat16 [4096, 19], P('group'), may hold values from -0.25 to 0.25
- acting_policy_logits: float32 [64, 63, 18], P('dp'), may hold values from -16 to 330, as said below
- actions: int32 [64, 63], P('dp'), may hold values from 0 to 17
- rewards: float32 [64, 63], P('dp'), may hold values from -6 to 6
- episode_finished: int32 [64, 63], P('dp'), may hold values 0 or 1
Outputs:
- trunk_grads: float32 [2, 4096, 4096], P(None, 'dp', 'group')
- head_grads: float32 [4096, 19], P(('group', 'dp'))
- actor_logits: float32 [1024, 18], P('dp')
The draws below stay inside these ranges and needn't reach their ends.
Inputs may be any that keep to these rules, and one draw needn't show every extreme that they name: `acting_policy_logits`: Real-valued scores, one row for each step and trajectory.
All inputs are finite; a program needn't handle non-finite values. No bound on the sum of `episode_finished` on one device may be relied on, other than what follows from the above.
Results may differ from the reference program's by a relative error of at most 0.012.
Values may be sent and summed in bfloat16 or wider, within the bound.
A program may use at most 128 MiB of HBM per device.

```python
import jax
import jax.numpy as jnp
from jax import lax

D = 4096
A = 18
HEADS = 19
LAYERS = 2
STEPS = 64
TRAJ = 64
ACTORS = 1024


def draw_acting_policy_logits(key, part):
    base_key = jax.random.fold_in(key, 11)
    first_key = jax.random.fold_in(base_key, 0)
    shape = (TRAJ, STEPS - 1, A)
    score_values = jnp.clip(3.0 * jax.random.normal(first_key, shape, jnp.float32), -15.0, 15.0)
    return score_values


def plant(entries, stream_key, low, top_value):
    dims = entries.shape
    spot = [jax.random.randint(jax.random.fold_in(stream_key, axis), (), 0, dims[axis]) for axis in range(len(dims))]
    entries = entries.at[tuple(spot)].set(low)
    longest = dims.index(max(dims))
    spot[longest] = (spot[longest] + 1) % dims[longest]
    return entries.at[tuple(spot)].set(top_value)


def block_scale(stream_key, shape, shards, smallest, top_value):
    level = 1.0
    for axis_at, parts in shards:
        draws = jax.random.uniform(jax.random.fold_in(jax.random.fold_in(stream_key, 6), axis_at), (parts,), jnp.float32, smallest / len(shards), top_value / len(shards))
        level = level * jnp.repeat(jnp.exp(draws), shape[axis_at] // parts).reshape((-1,) + (1,) * (len(shape) - 1 - axis_at))
    return level


def bell_draw(own_key, extent, deviation, limit, cuts=(), kind=jnp.bfloat16):
    array = jax.random.normal(own_key, extent, jnp.float32) * deviation
    if len(cuts) > 0:
        array = block_scale(own_key, extent, cuts, -0.22, 0.18) * array
    return jnp.clip(array, min=-limit, max=limit).astype(kind)


def setup_inputs(seed: int = 0) -> dict:
    key_of = jax.random.split(jax.random.key(seed), 9)
    observations = bell_draw(key_of[0], (TRAJ, STEPS, D), 1.0, 6.0, ((0, 8), (2, 4)))
    next_observations = bell_draw(key_of[1], (ACTORS, D), 1.0, 6.0, ((0, 8), (1, 4)))
    trunk_weights = bell_draw(key_of[2], (LAYERS, D, D), (D // 2) ** -0.5, 0.125, ((1, 8), (2, 4)))
    head_weights = bell_draw(key_of[3], (D, HEADS), (D // 9) ** -0.5, 0.25, ((0, 4),))
    acting_policy_logits = draw_acting_policy_logits(jax.random.fold_in(key_of[8], 71), 0)
    actions = plant(jax.random.randint(key_of[5], (TRAJ, STEPS - 1), 0, A), jax.random.fold_in(key_of[5], 1), 0, A - 1).astype(jnp.int32)
    rewards = bell_draw(key_of[6], (TRAJ, STEPS - 1), 1.0, 6.0, ((0, 8),), jnp.float32)
    episode_finished = plant((jax.random.randint(key_of[7], (TRAJ, STEPS - 1), 0, 16) < 1).astype(jnp.int32), jax.random.fold_in(key_of[7], 1), 0, 1)
    return dict(observations=observations, next_observations=next_observations, trunk_weights=trunk_weights, head_weights=head_weights, acting_policy_logits=acting_policy_logits, actions=actions, rewards=rewards, episode_finished=episode_finished)


discount_rate = 0.99
value_weight = 0.5
entropy_weight = 0.1
loss_divisor = 16.0


def contract_rows(left, right):
    return lax.dot_general(left, right, (((0,), (0,)), ((), ())), preferred_element_type=jnp.float32)


def contract_cols(left, right):
    return lax.dot_general(left, right, (((1,), (1,)), ((), ())), preferred_element_type=jnp.float32)


def silu_slope(pre_value):
    sigma = jax.nn.sigmoid(pre_value)
    return sigma * (1.0 + pre_value * (1.0 - sigma))


def importance_trace_gradients(learner_output, acting_policy_logits, actions, rewards, episode_finished):
    number_of_actions = acting_policy_logits.shape[-1]
    logits = learner_output[:, :, :number_of_actions]
    values = learner_output[:, :, number_of_actions]
    log_policy = jax.nn.log_softmax(logits[:, :-1], axis=-1)
    log_behave = jax.nn.log_softmax(acting_policy_logits, axis=-1)
    chosen = (actions[:, :, None] == jnp.arange(number_of_actions, dtype=jnp.int32)[None, None, :]).astype(jnp.float32)
    ratio = jnp.exp(jnp.sum((log_policy - log_behave) * chosen, axis=-1))
    clipped = jnp.minimum(ratio, 1.0)
    discount = discount_rate * (1.0 - episode_finished.astype(jnp.float32))
    current = values[:, :-1]
    following = values[:, 1:]
    deltas = clipped * (rewards + discount * following - current)

    def backward_step(carried, step_item):
        delta_now, factor_now = step_item
        carried = delta_now + factor_now * carried
        return carried, carried

    start_carry = jnp.zeros((values.shape[0],), jnp.float32)
    _, corrections = lax.scan(backward_step, start_carry, (deltas.T, (discount * clipped).T), reverse=True)
    targets = current + corrections.T
    next_targets = jnp.concatenate([targets[:, 1:], values[:, -1:]], axis=1)
    advantage = clipped * (rewards + discount * next_targets - current)
    probability = jnp.exp(log_policy)
    entropy = -jnp.sum(probability * log_policy, axis=-1)
    logit_grad = (-advantage[..., None] * (chosen - probability)
                  + entropy_weight * probability * (log_policy + entropy[..., None])) / loss_divisor
    value_grad = -value_weight * (targets - current) / loss_divisor
    step_grad = jnp.concatenate([logit_grad, value_grad[..., None]], axis=-1)
    last_row = jnp.zeros((values.shape[0], 1, number_of_actions + 1), jnp.float32)
    return jnp.concatenate([step_grad, last_row], axis=1)


def reference(observations, next_observations, trunk_weights, head_weights, acting_policy_logits, actions, rewards, episode_finished):
    traj_total, step_total, width = observations.shape
    learner_rows = traj_total * step_total
    number_of_actions = acting_policy_logits.shape[-1]
    layer_input = jnp.concatenate([observations.reshape(learner_rows, width), next_observations], axis=0)
    inputs_kept = []
    products_kept = []
    for layer_index in range(trunk_weights.shape[0]):
        inputs_kept.append(layer_input[:learner_rows])
        product = jnp.dot(layer_input, trunk_weights[layer_index], preferred_element_type=jnp.float32)
        products_kept.append(product[:learner_rows])
        layer_input = jax.nn.silu(product).astype(jnp.bfloat16)
    head_out = jnp.dot(layer_input, head_weights, preferred_element_type=jnp.float32)
    actor_logits = head_out[learner_rows:, :number_of_actions]
    learner_output = head_out[:learner_rows].reshape(traj_total, step_total, number_of_actions + 1)
    output_gradient = importance_trace_gradients(learner_output, acting_policy_logits, actions, rewards, episode_finished)
    output_gradient = output_gradient.reshape(learner_rows, number_of_actions + 1).astype(jnp.bfloat16)
    head_grads = contract_rows(layer_input[:learner_rows], output_gradient)
    input_grad = contract_cols(output_gradient, head_weights)
    layer_total = trunk_weights.shape[0]
    grad_list = [None] * layer_total
    for layer_index in range(layer_total - 1, -1, -1):
        pre_grad = (input_grad * silu_slope(products_kept[layer_index])).astype(jnp.bfloat16)
        grad_list[layer_index] = contract_rows(inputs_kept[layer_index], pre_grad)
        if layer_index > 0:
            input_grad = contract_cols(pre_grad, trunk_weights[layer_index])
    return jnp.stack(grad_list), head_grads, actor_logits
```

```python
import functools

import jax
import jax.numpy as jnp
from jax import lax
from jax.sharding import PartitionSpec as P

discount_rate = 0.99
value_weight = 0.5
entropy_weight = 0.1
loss_divisor = 16.0


def contract_rows(left, right):
    return lax.dot_general(
        left, right, (((0,), (0,)), ((), ())), preferred_element_type=jnp.float32
    )


def contract_cols(left, right):
    return lax.dot_general(
        left, right, (((1,), (1,)), ((), ())), preferred_element_type=jnp.float32
    )


def silu_slope(pre_value):
    sigma = jax.nn.sigmoid(pre_value)
    return sigma * (1.0 + pre_value * (1.0 - sigma))


def importance_trace_gradients(
    learner_output, acting_policy_logits, actions, rewards, episode_finished
):
    number_of_actions = acting_policy_logits.shape[-1]
    logits = learner_output[:, :, :number_of_actions]
    values = learner_output[:, :, number_of_actions]
    log_policy = jax.nn.log_softmax(logits[:, :-1], axis=-1)
    log_behave = jax.nn.log_softmax(acting_policy_logits, axis=-1)
    chosen = (
        actions[:, :, None] == jnp.arange(number_of_actions, dtype=jnp.int32)[None, None, :]
    ).astype(jnp.float32)
    ratio = jnp.exp(jnp.sum((log_policy - log_behave) * chosen, axis=-1))
    clipped = jnp.minimum(ratio, 1.0)
    discount = discount_rate * (1.0 - episode_finished.astype(jnp.float32))
    current = values[:, :-1]
    following = values[:, 1:]
    deltas = clipped * (rewards + discount * following - current)

    corrections, factors = deltas, discount * clipped
    reach, span = 1, deltas.shape[1]
    while reach < span:
        later = jnp.pad(corrections[:, reach:], ((0, 0), (0, reach)))
        later_factors = jnp.pad(factors[:, reach:], ((0, 0), (0, reach)))
        corrections = corrections + factors * later
        factors = factors * later_factors
        reach *= 2
    targets = current + corrections
    next_targets = jnp.concatenate([targets[:, 1:], values[:, -1:]], axis=1)
    advantage = clipped * (rewards + discount * next_targets - current)
    probability = jnp.exp(log_policy)
    entropy = -jnp.sum(probability * log_policy, axis=-1)
    logit_grad = (
        -advantage[..., None] * (chosen - probability)
        + entropy_weight * probability * (log_policy + entropy[..., None])
    ) / loss_divisor
    value_grad = -value_weight * (targets - current) / loss_divisor
    step_grad = jnp.concatenate([logit_grad, value_grad[..., None]], axis=-1)
    last_row = jnp.zeros((values.shape[0], 1, number_of_actions + 1), jnp.float32)
    return jnp.concatenate([step_grad, last_row], axis=1)


def swap(block, mask, size):
    return lax.ppermute(block, "group", [(index, index ^ mask) for index in range(size)])


def gather_features(block, size):
    if size != 4:
        return lax.all_gather(block, "group", axis=1, tiled=True)
    me = lax.axis_index("group")
    rows, width = block.shape
    half = rows // 2
    from_near = swap(block, 1, size)
    from_far = swap(block, 2, size)
    top = swap(from_near[:half], 2, size)
    bottom = swap(from_far[half:], 1, size)
    whole = jnp.zeros((rows, size * width), block.dtype)
    whole = lax.dynamic_update_slice(whole, block, (0, me * width))
    whole = lax.dynamic_update_slice(whole, from_near, (0, (me ^ 1) * width))
    whole = lax.dynamic_update_slice(whole, from_far, (0, (me ^ 2) * width))
    whole = lax.dynamic_update_slice(whole, top, (0, (me ^ 3) * width))
    return lax.dynamic_update_slice(whole, bottom, (half, (me ^ 3) * width))


def scatter_features(partial, size):
    if size != 4:
        return lax.psum_scatter(partial, "group", scatter_dimension=1, tiled=True)
    me = lax.axis_index("group")
    rows, width = partial.shape[0], partial.shape[1] // size
    half = rows // 2
    wire = jnp.bfloat16

    def part(start, mask):
        piece = lax.dynamic_slice(partial, (start, (me ^ mask) * width), (half, width))
        return piece

    def reduce_half(start, first, second):
        theirs = jnp.concatenate([part(start, first), part(start, 3)], axis=0)
        got = swap(theirs, first, size)
        onward = part(start, second).astype(jnp.float32) + got[half:].astype(jnp.float32)
        mine = part(start, 0).astype(jnp.float32) + got[:half].astype(jnp.float32)
        return mine + swap(onward.astype(wire), second, size).astype(jnp.float32)

    return jnp.concatenate([reduce_half(0, 1, 2), reduce_half(half, 2, 1)], axis=0)


def scatter_rows(block, size):
    if size & (size - 1):
        return lax.psum_scatter(block, "dp", scatter_dimension=0, tiled=True)
    me = lax.axis_index("dp")
    mask = size // 2
    while mask:
        half = block.shape[0] // 2
        upper = (me & mask) > 0
        theirs = jnp.where(upper, block[:half], block[half:])
        mine = jnp.where(upper, block[half:], block[:half])
        block = mine + lax.ppermute(theirs, "dp", [(i, i ^ mask) for i in range(size)])
        mask //= 2
    return block


def swap_cores(block, size):
    return lax.ppermute(block, "dp", [(index, index ^ 1) for index in range(size)])


def split_for_pair(whole, size):
    core = lax.axis_index("dp") % 2
    rows, width = whole.shape
    by_owner = whole.reshape(rows, size // 2, 2, width // size)

    def features_of(owner):
        picked = lax.dynamic_slice_in_dim(by_owner, owner, 1, axis=2)
        return picked.reshape(rows, width // 2)

    return features_of(core), swap_cores(features_of(1 - core), size)


def sum_group(block, size):
    if size != 4:
        return lax.psum(block, "group")
    block = block + swap(block, 1, size)
    return block + swap(block, 2, size)


def per_device(
    group_size,
    dp_size,
    observations,
    next_observations,
    trunk_weights,
    head_weights,
    acting_policy_logits,
    actions,
    rewards,
    episode_finished,
):
    traj_count, step_count, feature_block = observations.shape
    learner_rows = traj_count * step_count
    number_of_actions = acting_policy_logits.shape[-1]
    layer_total = trunk_weights.shape[0]
    own_rows = observations.reshape(learner_rows, feature_block)
    gathered_weights = [
        lax.all_gather(trunk_weights[layer_index], "dp", axis=0, tiled=True)
        for layer_index in range(layer_total)
    ]
    current = jnp.concatenate([own_rows, next_observations], axis=0)
    pair_inputs = []
    products_block = []
    for layer_index in range(layer_total):
        whole = gather_features(current, group_size)
        product = jnp.dot(
            whole, gathered_weights[layer_index], preferred_element_type=jnp.float32
        )
        pair_inputs.append(split_for_pair(whole[:learner_rows], dp_size))
        products_block.append(product[:learner_rows])
        current = jax.nn.silu(product).astype(jnp.bfloat16)
    partial_head = jnp.dot(current, head_weights, preferred_element_type=jnp.float32)
    totals = sum_group(partial_head, group_size)
    last_block = current[:learner_rows]
    head_out = totals[:learner_rows]
    actor_logits = totals[learner_rows:, :number_of_actions]
    learner_output = head_out.reshape(traj_count, step_count, number_of_actions + 1)
    output_gradient = importance_trace_gradients(
        learner_output, acting_policy_logits, actions, rewards, episode_finished
    )
    output_gradient = output_gradient.reshape(learner_rows, number_of_actions + 1).astype(
        jnp.bfloat16
    )
    input_grad = contract_cols(output_gradient, head_weights)
    grad_list = [None] * layer_total
    for layer_index in range(layer_total - 1, -1, -1):
        pre_grad = (input_grad * silu_slope(products_block[layer_index])).astype(jnp.bfloat16)
        near_inputs, far_inputs = pair_inputs[layer_index]
        far_grad = swap_cores(pre_grad, dp_size)
        partial = contract_rows(near_inputs, pre_grad) + contract_rows(far_inputs, far_grad)
        partial = partial.astype(jnp.bfloat16)
        partial, pre_grad = lax.optimization_barrier((partial, pre_grad))
        grad_list[layer_index] = lax.psum_scatter(
            partial,
            "dp",
            scatter_dimension=0,
            tiled=True,
            axis_index_groups=[list(range(core, dp_size, 2)) for core in range(2)],
        ).astype(jnp.float32)
        if layer_index > 0:
            full_grad = contract_cols(pre_grad, gathered_weights[layer_index]).astype(jnp.bfloat16)
            input_grad = scatter_features(full_grad, group_size)
    head_partial = contract_rows(last_block, output_gradient)
    head_grads = scatter_rows(head_partial, dp_size)
    return (jnp.stack(grad_list), head_grads, actor_logits)


def solution(mesh):
    in_specs = (
        P("dp", None, "group"),
        P("dp", "group"),
        P(None, "dp", "group"),
        P("group", None),
        P("dp", None, None),
        P("dp", None),
        P("dp", None),
        P("dp", None),
    )
    out_specs = (P(None, "dp", "group"), P(("group", "dp"), None), P("dp", None))
    return jax.shard_map(
        functools.partial(per_device, mesh.shape["group"], mesh.shape["dp"]),
        mesh=mesh, in_specs=in_specs, out_specs=out_specs, check_vma=False
    )
```
